512 devices in a mesh: dp: 16 (over z, core), expert: 8 (over y), sequence: 4 (over x).
Axes of the slice: x: 4, y: 8, z: 8, core: 2. Of those that a mesh axis runs over, the one named last changes fastest.
Arguments:
- tokens: bfloat16 [1536, 3072], P(('dp', 'sequence')), may hold values from -6 to 6
- cotangent: bfloat16 [1536, 3072], P(('dp', 'sequence')), may hold values from -4 to 4
- experts: int32 [1536, 2], P(('dp', 'sequence')), may hold values from 0 to 7, all different within a row; in each aligned block of 24 rows (0 to 23, 24 to 47, ...) at most 10 rows name the same one
- gate_weights: float32 [1536, 2], P(('dp', 'sequence')), may hold values from 0.1 to 1
- w_gate: bfloat16 [8, 8192, 3072], P('expert', ('dp', 'sequence')), may hold values from -0.109375 to 0.109375
- w_up: bfloat16 [8, 8192, 3072], P('expert', ('dp', 'sequence')), may hold values from -0.109375 to 0.109375
- w_down: bfloat16 [8, 8192, 3072], P('expert', ('dp', 'sequence')), may hold values from -0.0625 to 0.0625
Outputs:
- output: bfloat16 [1536, 3072], P(('dp', 'sequence'), 'expert')
- grad_tokens: bfloat16 [1536, 3072], P(('dp', 'sequence'), 'expert')
- grad_w_gate: bfloat16 [8, 8192, 3072], P('expert', ('dp', 'sequence'))
- grad_w_up: bfloat16 [8, 8192, 3072], P('expert', ('dp', 'sequence'))
- grad_w_down: bfloat16 [8, 8192, 3072], P('expert', ('dp', 'sequence'))
The draws below stay inside these ranges and needn't reach their ends.
Inputs may be any that keep to these rules, and one draw needn't show every extreme that they name: `experts`: A token's two ids differ. Within the rows of one device (aligned blocks of 24 rows) no id is named by more than 10 rows, a bound that some block reaches.
All inputs are finite; a program needn't handle non-finite values.
Results may differ from the reference program's by a relative error of at most 0.019.
Values may be sent and summed in bfloat16 or wider, within the bound.
No kernel may reach another device: no remote copies, remote signals or barrier semaphores. Data moves between devices by JAX's collectives and lax.ppermute only.
A program may use at most 128 MiB of HBM per device.

```python
import math
import jax
import jax.numpy as jnp
import numpy as np
from jax import lax

D = 3072
F = 8192
E = 8
TOK_DEV = 24
C = 10
TOKENS = 1536
N_DP = 16
N_SEQUENCE = 4


def block_scale(stream_key, extent, cuts, least, high):
    def one(dim, shards_of):
        steps = jax.random.uniform(jax.random.fold_in(jax.random.fold_in(stream_key, 6), dim), (shards_of,), jnp.float32, least / len(cuts), high / len(cuts))
        return jnp.repeat(jnp.exp(steps), extent[dim] // shards_of).reshape((-1,) + (1,) * (len(extent) - dim - 1))

    level = one(*cuts[0])
    for cut in cuts[1:]:
        level = level * one(*cut)
    return level


def deal_out(own_key, own, number, rows, count, top, most, skew):
    ranking = jax.random.permutation(own_key, count)
    packed, common = portions_of(count, rows * top, most, skew, True), portions_of(count, rows * top, most, skew, False)
    places = jnp.arange(count)

    def named(tallies, turn):
        used = int((tallies > 0).sum())
        fixed = max(1, used // 4)
        moved = fixed + (places - fixed + turn * (used - fixed)) % max(1, count - fixed)
        return jnp.zeros((count,), jnp.int32).at[ranking[jnp.where(places < fixed, places, moved)]].set(jnp.asarray(tallies, jnp.int32))

    tallies = jnp.where(number % 4 == 0, named(packed, number // 4), named(common, number - number // 4 - 1))
    mixed = jax.random.permutation(jax.random.fold_in(own, 3), count)
    donor, receiver = mixed[0:count // 2 * 2:2], mixed[1:count // 2 * 2:2]
    room = jnp.minimum(tallies[donor] - 1, most - tallies[receiver]) // 2
    room = jnp.where((donor == ranking[0]) | (receiver == ranking[0]) | (tallies[receiver] == 0), 0, jnp.maximum(room, 0))
    moved = jax.random.randint(jax.random.fold_in(own, 4), (count // 2,), 0, 1 << 20) % (room + 1)
    tallies = tallies.at[donor].add(-moved).at[receiver].add(moved)
    labels = jnp.searchsorted(jnp.cumsum(tallies), jnp.arange(rows * top), side="right").astype(jnp.int32)
    listing = labels.reshape(top, rows).T
    listing = listing[jax.random.permutation(jax.random.fold_in(own, 1), rows)]
    turn = jax.random.randint(jax.random.fold_in(own, 2), (rows, 1), 0, top)
    return jnp.take_along_axis(listing, (jnp.arange(top)[None, :] + turn) % top, axis=1)


def portions_of(count, total, bound, skew, full):
    weights = [(1 << 20) // math.isqrt(grade ** skew) + 1 for grade in range(1, count + 1)]
    largest = bound if full else min(bound, max(-(-total // count), total * weights[0] // sum(weights)))
    least = 1 if total - largest >= count - 1 else 0
    holding, spare = [largest] + [least] * (count - 1), total - largest - least * (count - 1)
    while spare > 0:
        candidates = [i for i in range(1, count) if holding[i] < largest] or [i for i in range(1, count) if holding[i] < bound]
        whole, left = sum([weights[i] for i in candidates]), spare
        for i in candidates:
            more = min(bound - holding[i], max(1, left * weights[i] // whole), spare)
            holding[i] = holding[i] + more
            spare = spare - more
    return np.array(holding)


def gaussian(key, dims, deviation, bound, shards=(), kind=jnp.bfloat16):
    array = jax.random.normal(key, dims, jnp.float32) * deviation
    if len(shards) > 0:
        array = block_scale(key, dims, shards, -0.22, 0.18) * array
    return jnp.clip(array, min=-bound, max=bound).astype(kind)


def setup_inputs(seed: int = 0) -> dict:
    key_list = jax.random.split(jax.random.key(seed), 8)
    tokens = gaussian(key_list[0], (TOKENS, D), 1.0, 6.0, ((0, 64),))
    cotangent = gaussian(key_list[1], (TOKENS, D), 0.5, 4.0, ((0, 64),))
    experts_keys = jax.random.split(jax.random.fold_in(key_list[2], 1), TOKENS // TOK_DEV)
    experts_turns = jax.random.permutation(jax.random.fold_in(key_list[2], 3), TOKENS // TOK_DEV)
    experts = jax.vmap(lambda own, number: deal_out(jax.random.fold_in(key_list[2], 2), own, number, TOK_DEV, E, 2, C, 2))(experts_keys, experts_turns).reshape((TOKENS, 2))
    gate_weights = jnp.clip(0.1 + 0.9 * jax.random.uniform(key_list[3], (TOKENS, 2), jnp.float32) ** block_scale(key_list[3], (TOKENS, 2), ((0, 64),), -0.2, 0.2), 0.1, 1.0)
    w_gate = gaussian(key_list[4], (E, F, D), D ** -0.5, 0.109375, ((0, 8), (1, 64)))
    w_up = gaussian(key_list[5], (E, F, D), D ** -0.5, 0.109375, ((0, 8), (1, 64)))
    w_down = gaussian(key_list[6], (E, F, D), F ** -0.5, 0.0625, ((0, 8), (1, 64)))
    return dict(tokens=tokens, cotangent=cotangent, experts=experts, gate_weights=gate_weights, w_gate=w_gate, w_up=w_up, w_down=w_down)


HIGH = lax.Precision.HIGHEST


def reference(tokens, cotangent, experts, gate_weights, w_gate, w_up, w_down):
    groups = N_DP * N_SEQUENCE
    routes_grouped = experts.reshape(groups, TOK_DEV, 2)
    gates_grouped = gate_weights.reshape(groups, TOK_DEV, 2)
    tok_grouped = tokens.astype(jnp.float32).reshape(groups, TOK_DEV, D)
    cot_grouped = cotangent.astype(jnp.float32).reshape(groups, TOK_DEV, D)
    slot_ids = jnp.arange(C, dtype=jnp.int32)
    width = F // N_DP
    out_sum = jnp.zeros((groups, TOK_DEV, D), jnp.float32)
    din_sum = jnp.zeros((groups, TOK_DEV, D), jnp.float32)
    grads_gate = []
    grads_up = []
    grads_down = []
    for expert in range(E):
        chosen = (routes_grouped == expert).astype(jnp.int32)
        routed = jnp.sum(chosen, axis=2)
        gate_of = jnp.sum(gates_grouped * chosen.astype(jnp.float32), axis=2)
        slot_of = jnp.cumsum(routed, axis=1) - routed
        placing = ((slot_of[:, None, :] == slot_ids[None, :, None]) & (routed[:, None, :] == 1)).astype(jnp.float32)
        slot_gate = jnp.einsum("gct,gt->gc", placing, gate_of, precision=HIGH)
        slot_tokens = jnp.einsum("gct,gtd->gcd", placing, tok_grouped, precision=HIGH).astype(jnp.bfloat16).reshape(groups * C, D)
        scaled_grad = jnp.einsum("gct,gtd->gcd", placing * gate_of[:, None, :], cot_grouped, precision=HIGH).astype(jnp.bfloat16).reshape(groups * C, D)
        pre_gate = jnp.dot(slot_tokens, w_gate[expert].T, preferred_element_type=jnp.float32)
        pre_up = jnp.dot(slot_tokens, w_up[expert].T, preferred_element_type=jnp.float32)
        sigmoid_gate = jax.nn.sigmoid(pre_gate)
        activated = pre_gate * sigmoid_gate
        hidden = (activated * pre_up).astype(jnp.bfloat16)
        hidden_sliced = hidden.astype(jnp.float32).reshape(groups * C, N_DP, width)
        down_sliced = w_down[expert].astype(jnp.float32).reshape(N_DP, width, D)
        pieces = jnp.einsum("rps,psd->prd", hidden_sliced, down_sliced, precision=HIGH)
        expert_out = jnp.sum(lax.optimization_barrier(pieces.astype(jnp.bfloat16)).astype(jnp.float32), axis=0)
        grad_hidden = jnp.dot(scaled_grad, w_down[expert].T, preferred_element_type=jnp.float32)
        grad_gate = (grad_hidden * pre_up * sigmoid_gate * (1.0 + pre_gate * (1.0 - sigmoid_gate))).astype(jnp.bfloat16)
        grad_up = (grad_hidden * activated).astype(jnp.bfloat16)
        din_pieces = jnp.einsum("rps,psd->prd", grad_gate.astype(jnp.float32).reshape(groups * C, N_DP, width), w_gate[expert].astype(jnp.float32).reshape(N_DP, width, D), precision=HIGH)
        din_pieces = din_pieces + jnp.einsum("rps,psd->prd", grad_up.astype(jnp.float32).reshape(groups * C, N_DP, width), w_up[expert].astype(jnp.float32).reshape(N_DP, width, D), precision=HIGH)
        expert_din = jnp.sum(lax.optimization_barrier(din_pieces.astype(jnp.bfloat16)).astype(jnp.float32), axis=0)
        out_sum = out_sum + jnp.einsum("gct,gcd->gtd", placing * slot_gate[:, :, None], expert_out.reshape(groups, C, D), precision=HIGH)
        din_sum = din_sum + jnp.einsum("gct,gcd->gtd", placing, expert_din.reshape(groups, C, D), precision=HIGH)
        grads_gate.append(jnp.dot(grad_gate.T, slot_tokens, preferred_element_type=jnp.float32).astype(jnp.bfloat16))
        grads_up.append(jnp.dot(grad_up.T, slot_tokens, preferred_element_type=jnp.float32).astype(jnp.bfloat16))
        grads_down.append(jnp.dot(hidden.T, scaled_grad, preferred_element_type=jnp.float32).astype(jnp.bfloat16))
    output = out_sum.reshape(TOKENS, D).astype(jnp.bfloat16)
    grad_tokens = din_sum.reshape(TOKENS, D).astype(jnp.bfloat16)
    return (output, grad_tokens, jnp.stack(grads_gate), jnp.stack(grads_up), jnp.stack(grads_down))
```

```python
import jax
import jax.numpy as jnp
from jax import lax
from jax.sharding import Mesh, PartitionSpec as P

C = 10
HIGH = lax.Precision.HIGHEST
F32 = jnp.float32
BF16 = jnp.bfloat16


def spread(block, axis):
    count = lax.axis_size(axis)
    copies = jnp.broadcast_to(block[None], (count,) + block.shape)
    return lax.all_to_all(copies, axis, split_axis=0, concat_axis=0, tiled=True)


def swap(a):
    return lax.ppermute(a, "c", [(0, 1), (1, 0)])


def slot_tables(experts, gate_weights, ids):
    chosen = (experts[:, :, None] == ids[None, None, :]).astype(jnp.int32)
    routed = jnp.sum(chosen, axis=1)
    gate_of = jnp.sum(gate_weights[:, :, None] * chosen.astype(F32), axis=1)
    slot_of = jnp.cumsum(routed, axis=0) - routed
    slot_ids = jnp.arange(C, dtype=jnp.int32)
    placing = (
        (slot_of.T[:, None, :] == slot_ids[None, :, None]) & (routed.T[:, None, :] == 1)
    ).astype(F32)
    return placing, gate_of


def dot(a, b, dims):
    return lax.dot_general(a, b, (dims, ((), ())), preferred_element_type=F32)


def forward_backward(rows_tok, rows_grad, w_gate, w_up, w_down):
    pre_gate = dot(rows_tok, w_gate, ((1,), (1,)))
    pre_up = dot(rows_tok, w_up, ((1,), (1,)))
    grad_hidden = dot(rows_grad, w_down, ((1,), (1,)))
    sigmoid_gate = jax.nn.sigmoid(pre_gate)
    activated = pre_gate * sigmoid_gate
    hidden = (activated * pre_up).astype(BF16)
    grad_gate = (
        grad_hidden * pre_up * sigmoid_gate * (1.0 + pre_gate * (1.0 - sigmoid_gate))
    ).astype(BF16)
    grad_up = (grad_hidden * activated).astype(BF16)
    out_part = dot(hidden, w_down, ((1,), (0,)))
    din_part = dot(grad_gate, w_gate, ((1,), (0,))) + dot(grad_up, w_up, ((1,), (0,)))
    return hidden, grad_gate, grad_up, out_part, din_part


def on_device(tokens, cotangent, experts, gate_weights, w_gate, w_up, w_down):
    w_gate, w_up, w_down = w_gate[0], w_up[0], w_down[0]
    width = tokens.shape[1]
    n_z, n_x, n_y = lax.axis_size("z"), lax.axis_size("x"), lax.axis_size("y")
    own_id = lax.axis_index("y")[None].astype(jnp.int32)
    placing, gate_of = slot_tables(experts, gate_weights, own_id)
    placing = placing[0]
    slot_gate = jnp.sum(placing * gate_of[:, 0][None, :], axis=1)
    picks = placing.astype(BF16)
    slot_tokens = dot(picks, tokens, ((1,), (0,))).astype(BF16)
    picked_grad = dot(picks, cotangent, ((1,), (0,)))
    scaled_grad = (picked_grad * slot_gate[:, None]).astype(BF16)

    block = jnp.concatenate([slot_tokens, scaled_grad], axis=0).reshape(4 * C, width // 2)
    by_z = spread(block, "z").reshape(n_z, 2, C, width)
    by_z = by_z.transpose(1, 0, 2, 3).reshape(2, n_z * C, width)
    own = spread(by_z, "x")
    other = swap(own)

    def rows(a, which):
        return a[:, which].reshape(n_x * n_z * C, width)

    tok_own, grad_own = rows(own, 0), rows(own, 1)
    tok_other, grad_other = rows(other, 0), rows(other, 1)
    hid_b, gg_b, gu_b, out_b, din_b = forward_backward(tok_other, grad_other, w_gate, w_up, w_down)
    hid_a, gg_a, gu_a, out_a, din_a = forward_backward(tok_own, grad_own, w_gate, w_up, w_down)

    def pack(out_part, din_part):
        return jnp.stack(
            [
                out_part.reshape(n_x, n_z * C, width),
                din_part.reshape(n_x, n_z * C, width),
            ],
            axis=1,
        )

    from_partner = swap(pack(out_b.astype(BF16), din_b.astype(BF16)))
    chip_sum = (pack(out_a, din_a) + from_partner.astype(F32)).astype(BF16)

    def weight_grad(left_a, right_a, left_b, right_b):
        total = dot(left_a, right_a, ((0,), (0,))) + dot(left_b, right_b, ((0,), (0,)))
        return total.astype(BF16)[None]

    grad_w_gate = weight_grad(gg_a, tok_own, gg_b, tok_other)
    grad_w_up = weight_grad(gu_a, tok_own, gu_b, tok_other)
    grad_w_down = weight_grad(hid_a, grad_own, hid_b, grad_other)

    sum_x = lax.all_to_all(chip_sum, "x", split_axis=0, concat_axis=0, tiled=True)
    sum_x = jnp.sum(sum_x.astype(F32), axis=0).astype(BF16)
    sum_x = sum_x.reshape(2, n_z, C, width).transpose(1, 0, 2, 3).reshape(n_z, 4 * C, width // 2)
    sum_z = lax.all_to_all(sum_x, "z", split_axis=0, concat_axis=0, tiled=True)
    sum_z = jnp.sum(sum_z.astype(F32), axis=0).astype(BF16)
    part = width // n_y
    to_y = sum_z.reshape(2 * C, n_y, part).transpose(1, 0, 2)
    by_y = lax.all_to_all(to_y, "y", split_axis=0, concat_axis=0, tiled=True)
    by_y = by_y.reshape(n_y, 2, C, part).astype(F32)

    all_placing, all_gates = slot_tables(
        experts, gate_weights, jnp.arange(n_y, dtype=jnp.int32)
    )
    weighted = all_placing * all_gates.T[:, None, :]
    output = jnp.einsum("ect,ecd->td", weighted, by_y[:, 0], precision=HIGH)
    grad_tokens = jnp.einsum("ect,ecd->td", all_placing, by_y[:, 1], precision=HIGH)
    return (
        output.astype(BF16),
        grad_tokens.astype(BF16),
        grad_w_gate,
        grad_w_up,
        grad_w_down,
    )


def solution(mesh):
    shape = mesh.devices.shape
    fine = Mesh(
        mesh.devices.reshape(shape[0] // 2, 2, shape[1], shape[2]), ("z", "c", "y", "x")
    )
    by_token = ("z", "c", "x")
    return jax.shard_map(
        on_device,
        mesh=fine,
        in_specs=(
            P(by_token, None),
            P(by_token, None),
            P(by_token, None),
            P(by_token, None),
            P("y", by_token, None),
            P("y", by_token, None),
            P("y", by_token, None),
        ),
        out_specs=(
            P(by_token, "y"),
            P(by_token, "y"),
            P("y", by_token, None),
            P("y", by_token, None),
            P("y", by_token, None),
        ),
        check_vma=False,
    )
```

```python
import jax
import jax.numpy as jnp
from jax import lax
from jax.sharding import Mesh, PartitionSpec as P

C = 10
HIGH = lax.Precision.HIGHEST
F32 = jnp.float32
BF16 = jnp.bfloat16


def spread(block, axis):
    count = lax.axis_size(axis)
    copies = jnp.broadcast_to(block[None], (count,) + block.shape)
    return lax.all_to_all(copies, axis, split_axis=0, concat_axis=0, tiled=True)


def swap(a):
    return lax.ppermute(a, "c", [(0, 1), (1, 0)])


def slot_tables(experts, gate_weights, ids):
    chosen = (experts[:, :, None] == ids[None, None, :]).astype(jnp.int32)
    routed = jnp.sum(chosen, axis=1)
    gate_of = jnp.sum(gate_weights[:, :, None] * chosen.astype(F32), axis=1)
    slot_of = jnp.cumsum(routed, axis=0) - routed
    slot_ids = jnp.arange(C, dtype=jnp.int32)
    placing = (
        (slot_of.T[:, None, :] == slot_ids[None, :, None]) & (routed.T[:, None, :] == 1)
    ).astype(F32)
    return placing, gate_of


def dot(a, b, dims):
    return lax.dot_general(a, b, (dims, ((), ())), preferred_element_type=F32)


def dot2(rows, w):
    return dot(rows[0], w[0], ((1,), (1,))) + dot(rows[1], w[1], ((1,), (1,)))


def forward_backward(rows_tok, rows_grad, w_gate, w_up, w_down):
    pre_gate = dot2(rows_tok, w_gate)
    pre_up = dot2(rows_tok, w_up)
    grad_hidden = dot2(rows_grad, w_down)
    sigmoid_gate = jax.nn.sigmoid(pre_gate)
    activated = pre_gate * sigmoid_gate
    hidden = (activated * pre_up).astype(BF16)
    grad_gate = (
        grad_hidden * pre_up * sigmoid_gate * (1.0 + pre_gate * (1.0 - sigmoid_gate))
    ).astype(BF16)
    grad_up = (grad_hidden * activated).astype(BF16)
    out_part = [dot(hidden, w_down[i], ((1,), (0,))) for i in range(2)]
    din_part = [
        dot(grad_gate, w_gate[i], ((1,), (0,))) + dot(grad_up, w_up[i], ((1,), (0,)))
        for i in range(2)
    ]
    return hidden, grad_gate, grad_up, out_part, din_part


def on_device(tokens, cotangent, experts, gate_weights, w_gate, w_up, w_down):
    w_gate, w_up, w_down = w_gate[0], w_up[0], w_down[0]
    width = tokens.shape[1]
    n_z, n_x, n_y = lax.axis_size("z"), lax.axis_size("x"), lax.axis_size("y")
    own_id = lax.axis_index("y")[None].astype(jnp.int32)
    placing, gate_of = slot_tables(experts, gate_weights, own_id)
    placing = placing[0]
    slot_gate = jnp.sum(placing * gate_of[:, 0][None, :], axis=1)
    picks = placing.astype(BF16)
    slot_tokens = dot(picks, tokens, ((1,), (0,))).astype(BF16)
    picked_grad = dot(picks, cotangent, ((1,), (0,)))
    scaled_grad = (picked_grad * slot_gate[:, None]).astype(BF16)

    share = width // 2
    tail = width - share
    block = jnp.concatenate([slot_tokens, scaled_grad], axis=0)
    n_rows = n_x * n_z * C

    first = spread(block[:, :share].reshape(4 * C, share // 2), "z").reshape(n_z, 2, C, share)
    first = first.transpose(1, 0, 2, 3).reshape(2, n_z * C, share)
    last = spread(block[:, share:].reshape(4 * C, tail // 2), "x").reshape(n_x, 2, C, tail)
    last = last.transpose(1, 0, 2, 3).reshape(2, n_x * C, tail)
    first = spread(first, "x")
    last = lax.all_gather(last, "z", axis=0)
    first_other, last_other = swap(first), swap(last)

    at_x = lax.broadcasted_iota(jnp.int32, (n_rows, n_rows), 0)
    at_z = lax.broadcasted_iota(jnp.int32, (n_rows, n_rows), 1)
    of_z, of_x, of_slot = at_z // (n_x * C), at_z // C % n_x, at_z % C
    turn = (at_x == of_x * (n_z * C) + of_z * C + of_slot).astype(BF16)

    def rows(head, rest, which):
        rest = dot(turn, rest[:, which].reshape(n_rows, tail), ((1,), (0,))).astype(BF16)
        return head[:, which].reshape(n_rows, share), rest

    tok_own, grad_own = rows(first, last, 0), rows(first, last, 1)
    tok_other, grad_other = rows(first_other, last_other, 0), rows(first_other, last_other, 1)
    weights = [(w[:, :share], w[:, share:]) for w in (w_gate, w_up, w_down)]
    hid_b, gg_b, gu_b, out_b, din_b = forward_backward(tok_other, grad_other, *weights)
    hid_a, gg_a, gu_a, out_a, din_a = forward_backward(tok_own, grad_own, *weights)

    def pack(out_part, din_part, outer):
        return jnp.stack(
            [a.reshape(outer, n_rows // outer, a.shape[1]) for a in (out_part, din_part)], axis=1
        )

    def chip_sum(mine, partner, outer):
        partner = swap(pack(*[a.astype(BF16) for a in partner], outer))
        return (pack(*mine, outer) + partner.astype(F32)).astype(BF16)

    sum_first = chip_sum((out_a[0], din_a[0]), (out_b[0], din_b[0]), n_x)

    def turned(a):
        return dot(turn, a, ((0,), (0,))).astype(BF16)

    sum_last = chip_sum((out_a[1], din_a[1]), (out_b[1], din_b[1]), 1)[0]
    sum_last = pack(turned(sum_last[0]), turned(sum_last[1]), n_z)

    def weight_grad(left_a, right_a, left_b, right_b):
        parts = [
            dot(left_a, right_a[i], ((0,), (0,))) + dot(left_b, right_b[i], ((0,), (0,)))
            for i in range(2)
        ]
        return jnp.concatenate([p.astype(BF16) for p in parts], axis=1)[None]

    grad_w_gate = weight_grad(gg_a, tok_own, gg_b, tok_other)
    grad_w_up = weight_grad(gu_a, tok_own, gu_b, tok_other)
    grad_w_down = weight_grad(hid_a, grad_own, hid_b, grad_other)

    def exchange_sum(a, axis):
        a = lax.all_to_all(a, axis, split_axis=0, concat_axis=0, tiled=True)
        return jnp.sum(a.astype(F32), axis=0).astype(BF16)

    def by_block(a, count):
        wide = a.shape[-1]
        a = a.reshape(2, count, C, wide).transpose(1, 0, 2, 3)
        return a.reshape(count, 4 * C, wide // 2)

    sum_last = lax.psum_scatter(sum_last, "z", scatter_dimension=0, tiled=False)
    sum_first = exchange_sum(sum_first, "x")
    sum_first = exchange_sum(by_block(sum_first, n_z), "z").reshape(2 * C, share)
    sum_last = exchange_sum(by_block(sum_last, n_x), "x").reshape(2 * C, tail)
    sum_z = jnp.concatenate([sum_first, sum_last], axis=1)
    part = width // n_y
    to_y = sum_z.reshape(2 * C, n_y, part).transpose(1, 0, 2)
    by_y = lax.all_to_all(to_y, "y", split_axis=0, concat_axis=0, tiled=True)
    by_y = by_y.reshape(n_y, 2, C, part).astype(F32)

    all_placing, all_gates = slot_tables(
        experts, gate_weights, jnp.arange(n_y, dtype=jnp.int32)
    )
    weighted = all_placing * all_gates.T[:, None, :]
    output = jnp.einsum("ect,ecd->td", weighted, by_y[:, 0], precision=HIGH)
    grad_tokens = jnp.einsum("ect,ecd->td", all_placing, by_y[:, 1], precision=HIGH)
    return (
        output.astype(BF16),
        grad_tokens.astype(BF16),
        grad_w_gate,
        grad_w_up,
        grad_w_down,
    )


def solution(mesh):
    shape = mesh.devices.shape
    fine = Mesh(
        mesh.devices.reshape(shape[0] // 2, 2, shape[1], shape[2]), ("z", "c", "y", "x")
    )
    by_token = ("z", "c", "x")
    return jax.shard_map(
        on_device,
        mesh=fine,
        in_specs=(
            P(by_token, None),
            P(by_token, None),
            P(by_token, None),
            P(by_token, None),
            P("y", by_token, None),
            P("y", by_token, None),
            P("y", by_token, None),
        ),
        out_specs=(
            P(by_token, "y"),
            P(by_token, "y"),
            P("y", by_token, None),
            P("y", by_token, None),
            P("y", by_token, None),
        ),
        check_vma=False,
    )
```

```python
import jax
import jax.numpy as jnp
from jax import lax
from jax.sharding import Mesh, PartitionSpec as P

C = 10
HIGH = lax.Precision.HIGHEST
F32 = jnp.float32
BF16 = jnp.bfloat16


def spread(block, axis):
    count = lax.axis_size(axis)
    copies = jnp.broadcast_to(block[None], (count,) + block.shape)
    return lax.all_to_all(copies, axis, split_axis=0, concat_axis=0, tiled=True)


def swap(a):
    return lax.ppermute(a, "c", [(0, 1), (1, 0)])


def slot_tables(experts, gate_weights, ids):
    chosen = (experts[:, :, None] == ids[None, None, :]).astype(jnp.int32)
    routed = jnp.sum(chosen, axis=1)
    gate_of = jnp.sum(gate_weights[:, :, None] * chosen.astype(F32), axis=1)
    slot_of = jnp.cumsum(routed, axis=0) - routed
    slot_ids = jnp.arange(C, dtype=jnp.int32)
    placing = (
        (slot_of.T[:, None, :] == slot_ids[None, :, None]) & (routed.T[:, None, :] == 1)
    ).astype(F32)
    return placing, gate_of


def dot(a, b, dims):
    return lax.dot_general(a, b, (dims, ((), ())), preferred_element_type=F32)


def shift(a, step):
    count = lax.axis_size("z")
    return lax.ppermute(a, "z", [(i, (i + step) % count) for i in range(count)])


def ring_gather(block, ahead):
    up, down, from_below, from_above = block, block, [], []
    for step in range(ahead):
        up = shift(up, 1)
        from_below.append(up)
        if step < lax.axis_size("z") - 1 - ahead:
            down = shift(down, -1)
            from_above.append(down)
    return jnp.concatenate([block] + from_below + from_above[::-1], axis=0)


def ring_sum(parts, ahead):
    count = len(parts)
    down, up = parts[ahead], parts[ahead + 1]
    for step in range(ahead):
        down = shift(down, -1)
        if step < ahead - 1:
            down = (down.astype(F32) + parts[ahead - 1 - step].astype(F32)).astype(BF16)
        if step < count - 1 - ahead:
            up = shift(up, 1)
            if step < count - 2 - ahead:
                up = (up.astype(F32) + parts[ahead + 2 + step].astype(F32)).astype(BF16)
    return (parts[0].astype(F32) + down.astype(F32) + up.astype(F32)).astype(BF16)


def forward_backward(rows_tok, rows_grad, w_gate, w_up, w_down, turn):
    pre_gate = dot(rows_tok, w_gate, ((1,), (1,)))
    pre_up = dot(rows_tok, w_up, ((1,), (1,)))
    grad_hidden = dot(rows_grad, w_down, ((1,), (1,)))
    grad_hidden = jnp.dot(turn, grad_hidden, precision=HIGH)
    sigmoid_gate = jax.nn.sigmoid(pre_gate)
    activated = pre_gate * sigmoid_gate
    hidden = (activated * pre_up).astype(BF16)
    grad_gate = (
        grad_hidden * pre_up * sigmoid_gate * (1.0 + pre_gate * (1.0 - sigmoid_gate))
    ).astype(BF16)
    grad_up = (grad_hidden * activated).astype(BF16)
    out_part = dot(hidden, w_down, ((1,), (0,)))
    turned = [
        dot(turn.astype(BF16), a, ((0,), (0,))).astype(BF16) for a in (hidden, grad_gate, grad_up)
    ]
    din_part = dot(turned[1], w_gate, ((1,), (0,))) + dot(turned[2], w_up, ((1,), (0,)))
    return turned[0], grad_gate, grad_up, out_part, din_part


def on_device(tokens, cotangent, experts, gate_weights, w_gate, w_up, w_down):
    w_gate, w_up, w_down = w_gate[0], w_up[0], w_down[0]
    width = tokens.shape[1]
    n_z, n_x, n_y = lax.axis_size("z"), lax.axis_size("x"), lax.axis_size("y")
    own_id = lax.axis_index("y")[None].astype(jnp.int32)
    placing, gate_of = slot_tables(experts, gate_weights, own_id)
    placing = placing[0]
    slot_gate = jnp.sum(placing * gate_of[:, 0][None, :], axis=1)
    picks = placing.astype(BF16)
    slot_tokens = dot(picks, tokens, ((1,), (0,))).astype(BF16)
    picked_grad = dot(picks, cotangent, ((1,), (0,)))
    scaled_grad = (picked_grad * slot_gate[:, None]).astype(BF16)

    n_rows = n_x * n_z * C
    quarter = (4 * C, width // 4)
    tok_own = spread(slot_tokens.reshape(quarter), "z").reshape(n_z * C, width)
    grad_own = spread(scaled_grad.reshape(quarter), "x").reshape(n_x * C, width)
    tok_own = spread(tok_own, "x").reshape(n_rows, width)
    ahead = n_z // 2
    grad_own = ring_gather(grad_own, ahead)
    tok_other, grad_other = swap(tok_own), swap(grad_own)

    at_tok = lax.broadcasted_iota(jnp.int32, (n_rows, n_rows), 0)
    at_grad = lax.broadcasted_iota(jnp.int32, (n_rows, n_rows), 1)
    of_z = (lax.axis_index("z") - at_grad // (n_x * C) + n_z) % n_z
    of_x, of_slot = at_grad // C % n_x, at_grad % C
    turn = (at_tok == of_x * (n_z * C) + of_z * C + of_slot).astype(F32)

    weights = (w_gate, w_up, w_down, turn)
    hid_b, gg_b, gu_b, out_b, din_b = forward_backward(tok_other, grad_other, *weights)
    hid_a, gg_a, gu_a, out_a, din_a = forward_backward(tok_own, grad_own, *weights)

    def chip_sum(mine, partner):
        return (mine + swap(partner.astype(BF16)).astype(F32)).astype(BF16)

    sum_out = chip_sum(out_a, out_b).reshape(n_x, n_z * C, width)
    sum_din = chip_sum(din_a, din_b).reshape(n_z, n_x * C, width)

    def weight_grad(left_a, right_a, left_b, right_b):
        total = dot(left_a, right_a, ((0,), (0,))) + dot(left_b, right_b, ((0,), (0,)))
        return total.astype(BF16)[None]

    grad_w_gate = weight_grad(gg_a, tok_own, gg_b, tok_other)
    grad_w_up = weight_grad(gu_a, tok_own, gu_b, tok_other)
    grad_w_down = weight_grad(hid_a, grad_own, hid_b, grad_other)

    def exchange_sum(a, axis):
        a = lax.all_to_all(a, axis, split_axis=0, concat_axis=0, tiled=True)
        return jnp.sum(a.astype(F32), axis=0).astype(BF16)

    sum_out = exchange_sum(sum_out, "x")
    sum_din = ring_sum([sum_din[j] for j in range(n_z)], ahead)
    sum_out = exchange_sum(sum_out.reshape((n_z,) + quarter), "z").reshape(C, width)
    sum_din = exchange_sum(sum_din.reshape((n_x,) + quarter), "x").reshape(C, width)
    sum_z = jnp.concatenate([sum_out, sum_din], axis=0)
    part = width // n_y
    to_y = sum_z.reshape(2 * C, n_y, part).transpose(1, 0, 2)
    by_y = lax.all_to_all(to_y, "y", split_axis=0, concat_axis=0, tiled=True)
    by_y = by_y.reshape(n_y, 2, C, part).astype(F32)

    all_placing, all_gates = slot_tables(
        experts, gate_weights, jnp.arange(n_y, dtype=jnp.int32)
    )
    weighted = all_placing * all_gates.T[:, None, :]
    output = jnp.einsum("ect,ecd->td", weighted, by_y[:, 0], precision=HIGH)
    grad_tokens = jnp.einsum("ect,ecd->td", all_placing, by_y[:, 1], precision=HIGH)
    return (
        output.astype(BF16),
        grad_tokens.astype(BF16),
        grad_w_gate,
        grad_w_up,
        grad_w_down,
    )


def solution(mesh):
    shape = mesh.devices.shape
    fine = Mesh(
        mesh.devices.reshape(shape[0] // 2, 2, shape[1], shape[2]), ("z", "c", "y", "x")
    )
    by_token = ("z", "c", "x")
    return jax.shard_map(
        on_device,
        mesh=fine,
        in_specs=(
            P(by_token, None),
            P(by_token, None),
            P(by_token, None),
            P(by_token, None),
            P("y", by_token, None),
            P("y", by_token, None),
            P("y", by_token, None),
        ),
        out_specs=(
            P(by_token, "y"),
            P(by_token, "y"),
            P("y", by_token, None),
            P("y", by_token, None),
            P("y", by_token, None),
        ),
        check_vma=False,
    )
```

```python
import jax
import jax.numpy as jnp
from jax import lax
from jax.experimental import pallas as pl
from jax.experimental.pallas import tpu as pltpu
from jax.sharding import Mesh, PartitionSpec as P

C = 10
HIGH = lax.Precision.HIGHEST
F32 = jnp.float32
BF16 = jnp.bfloat16


def spread(block, axis):
    count = lax.axis_size(axis)
    copies = jnp.broadcast_to(block[None], (count,) + block.shape)
    return lax.all_to_all(copies, axis, split_axis=0, concat_axis=0, tiled=True)


def swap(a):
    return lax.ppermute(a, "c", [(0, 1), (1, 0)])


def slot_tables(experts, gate_weights, ids):
    chosen = (experts[:, :, None] == ids[None, None, :]).astype(jnp.int32)
    routed = jnp.sum(chosen, axis=1)
    gate_of = jnp.sum(gate_weights[:, :, None] * chosen.astype(F32), axis=1)
    slot_of = jnp.cumsum(routed, axis=0) - routed
    slot_ids = jnp.arange(C, dtype=jnp.int32)
    placing = (
        (slot_of.T[:, None, :] == slot_ids[None, :, None]) & (routed.T[:, None, :] == 1)
    ).astype(F32)
    return placing, gate_of


def dot(a, b, dims):
    return lax.dot_general(a, b, (dims, ((), ())), preferred_element_type=F32)


def layer_kernel(tok_ref, grad_ref, wg_ref, wu_ref, wd_ref, turn_ref, *outs):
    turned_hidden_ref, grad_gate_ref, grad_up_ref, out_ref, din_ref = outs
    w_gate, w_up, w_down = wg_ref[...], wu_ref[...], wd_ref[...]
    turn = turn_ref[...]
    units = w_gate.shape[0]
    rows_tok = tok_ref[...]
    grad_hidden = dot(grad_ref[...], w_down, ((1,), (1,)))
    high = grad_hidden.astype(BF16)
    rest = grad_hidden - high.astype(F32)
    middle = rest.astype(BF16)
    low = (rest - middle.astype(F32)).astype(BF16)
    pieces = dot(turn, jnp.concatenate([high, middle, low], axis=1), ((1,), (0,)))
    grad_hidden = (
        pieces[:, :units] + pieces[:, units : 2 * units] + pieces[:, 2 * units :]
    )
    pre_gate = dot(rows_tok, w_gate, ((1,), (1,)))
    pre_up = dot(rows_tok, w_up, ((1,), (1,)))
    sigmoid_gate = jax.nn.sigmoid(pre_gate)
    activated = pre_gate * sigmoid_gate
    hidden = (activated * pre_up).astype(BF16)
    grad_gate = (
        grad_hidden * pre_up * sigmoid_gate * (1.0 + pre_gate * (1.0 - sigmoid_gate))
    ).astype(BF16)
    grad_up = (grad_hidden * activated).astype(BF16)
    grad_gate_ref[...] = grad_gate
    grad_up_ref[...] = grad_up
    turned = dot(turn, jnp.concatenate([hidden, grad_gate, grad_up], axis=1), ((0,), (0,)))
    turned = turned.astype(BF16)
    turned_hidden_ref[...] = turned[:, :units]
    din_part = dot(turned[:, units : 2 * units], w_gate, ((1,), (0,)))
    din_part += dot(turned[:, 2 * units :], w_up, ((1,), (0,)))
    din_ref[...] = din_part.astype(BF16)
    out_ref[...] = dot(hidden, w_down, ((1,), (0,))).astype(BF16)


def forward_backward(rows_tok, rows_grad, w_gate, w_up, w_down, turn):
    n_rows, width = rows_tok.shape
    narrow = jax.ShapeDtypeStruct((n_rows, w_gate.shape[0]), BF16)
    wide = jax.ShapeDtypeStruct((n_rows, width), BF16)
    return pl.pallas_call(
        layer_kernel,
        out_shape=(narrow, narrow, narrow, wide, wide),
        compiler_params=pltpu.CompilerParams(vmem_limit_bytes=40 * 1024 * 1024),
        name="layer",
    )(rows_tok, rows_grad, w_gate, w_up, w_down, turn)


def on_device(tokens, cotangent, experts, gate_weights, w_gate, w_up, w_down):
    w_gate, w_up, w_down = w_gate[0], w_up[0], w_down[0]
    width = tokens.shape[1]
    n_z, n_x, n_y = lax.axis_size("z"), lax.axis_size("x"), lax.axis_size("y")
    own_id = lax.axis_index("y")[None].astype(jnp.int32)
    placing, gate_of = slot_tables(experts, gate_weights, own_id)
    placing = placing[0]
    slot_gate = jnp.sum(placing * gate_of[:, 0][None, :], axis=1)
    picks = placing.astype(BF16)
    slot_tokens = dot(picks, tokens, ((1,), (0,))).astype(BF16)
    picked_grad = dot(picks, cotangent, ((1,), (0,)))
    scaled_grad = (picked_grad * slot_gate[:, None]).astype(BF16)

    n_rows = n_x * n_z * C
    quarter = (4 * C, width // 4)
    grad_own = spread(scaled_grad.reshape(quarter), "x").reshape(n_x * C, width)
    grad_own = lax.all_gather(grad_own, "z", axis=0, tiled=True)
    tok_own = spread(slot_tokens.reshape(quarter), "z").reshape(n_z * C, width)
    tok_own = spread(tok_own, "x").reshape(n_rows, width)
    tok_other, grad_other = swap(tok_own), swap(grad_own)

    at_tok = lax.broadcasted_iota(jnp.int32, (n_rows, n_rows), 0)
    at_grad = lax.broadcasted_iota(jnp.int32, (n_rows, n_rows), 1)
    of_z, of_x, of_slot = at_grad // (n_x * C), at_grad // C % n_x, at_grad % C
    turn = (at_tok == of_x * (n_z * C) + of_z * C + of_slot).astype(BF16)

    weights = (w_gate, w_up, w_down, turn)
    hid_b, gg_b, gu_b, out_b, din_b = forward_backward(tok_other, grad_other, *weights)
    hid_a, gg_a, gu_a, out_a, din_a = forward_backward(tok_own, grad_own, *weights)

    def chip_sum(mine, partner):
        return (mine.astype(F32) + swap(partner).astype(F32)).astype(BF16)

    sum_din = chip_sum(din_a, din_b)
    sum_out = chip_sum(out_a, out_b).reshape(n_x, n_z * C, width)

    def weight_grad(left_a, right_a, left_b, right_b):
        total = dot(left_a, right_a, ((0,), (0,))) + dot(left_b, right_b, ((0,), (0,)))
        return total.astype(BF16)[None]

    grad_w_gate = weight_grad(gg_a, tok_own, gg_b, tok_other)
    grad_w_up = weight_grad(gu_a, tok_own, gu_b, tok_other)
    grad_w_down = weight_grad(hid_a, grad_own, hid_b, grad_other)

    def exchange_sum(a, axis):
        a = lax.all_to_all(a, axis, split_axis=0, concat_axis=0, tiled=True)
        return jnp.sum(a.astype(F32), axis=0).astype(BF16)

    sum_din = lax.psum_scatter(sum_din, "z", scatter_dimension=0, tiled=True)
    sum_out = exchange_sum(sum_out, "x")
    sum_out = exchange_sum(sum_out.reshape((n_z,) + quarter), "z").reshape(C, width)
    sum_din = exchange_sum(sum_din.reshape((n_x,) + quarter), "x").reshape(C, width)
    sum_z = jnp.concatenate([sum_out, sum_din], axis=0)
    part = width // n_y
    to_y = sum_z.reshape(2 * C, n_y, part).transpose(1, 0, 2)
    by_y = lax.all_to_all(to_y, "y", split_axis=0, concat_axis=0, tiled=True)
    by_y = by_y.reshape(n_y, 2, C, part).astype(F32)

    all_placing, all_gates = slot_tables(
        experts, gate_weights, jnp.arange(n_y, dtype=jnp.int32)
    )
    weighted = all_placing * all_gates.T[:, None, :]
    output = jnp.einsum("ect,ecd->td", weighted, by_y[:, 0], precision=HIGH)
    grad_tokens = jnp.einsum("ect,ecd->td", all_placing, by_y[:, 1], precision=HIGH)
    return (
        output.astype(BF16),
        grad_tokens.astype(BF16),
        grad_w_gate,
        grad_w_up,
        grad_w_down,
    )


def solution(mesh):
    shape = mesh.devices.shape
    fine = Mesh(
        mesh.devices.reshape(shape[0] // 2, 2, shape[1], shape[2]), ("z", "c", "y", "x")
    )
    by_token = ("z", "c", "x")
    return jax.shard_map(
        on_device,
        mesh=fine,
        in_specs=(
            P(by_token, None),
            P(by_token, None),
            P(by_token, None),
            P(by_token, None),
            P("y", by_token, None),
            P("y", by_token, None),
            P("y", by_token, None),
        ),
        out_specs=(
            P(by_token, "y"),
            P(by_token, "y"),
            P("y", by_token, None),
            P("y", by_token, None),
            P("y", by_token, None),
        ),
        check_vma=False,
    )
```

```python
import jax
import jax.numpy as jnp
from jax import lax
from jax.experimental import pallas as pl
from jax.experimental.pallas import tpu as pltpu
from jax.sharding import Mesh, PartitionSpec as P

C = 10
HIGH = lax.Precision.HIGHEST
F32 = jnp.float32
BF16 = jnp.bfloat16


def spread(block, axis):
    count = lax.axis_size(axis)
    copies = jnp.broadcast_to(block[None], (count,) + block.shape)
    return lax.all_to_all(copies, axis, split_axis=0, concat_axis=0, tiled=True)


def swap(a):
    return lax.ppermute(a, "c", [(0, 1), (1, 0)])


def slot_tables(experts, gate_weights, ids):
    chosen = (experts[:, :, None] == ids[None, None, :]).astype(jnp.int32)
    routed = jnp.sum(chosen, axis=1)
    gate_of = jnp.sum(gate_weights[:, :, None] * chosen.astype(F32), axis=1)
    slot_of = jnp.cumsum(routed, axis=0) - routed
    slot_ids = jnp.arange(C, dtype=jnp.int32)
    placing = (
        (slot_of.T[:, None, :] == slot_ids[None, :, None]) & (routed.T[:, None, :] == 1)
    ).astype(F32)
    return placing, gate_of


def dot(a, b, dims):
    return lax.dot_general(a, b, (dims, ((), ())), preferred_element_type=F32)


def layer_kernel(tok_ref, grad_ref, wg_ref, wu_ref, wd_ref, turn_ref, *outs):
    turned_hidden_ref, grad_gate_ref, grad_up_ref, out_ref, din_ref = outs
    w_gate, w_up, w_down = wg_ref[...], wu_ref[...], wd_ref[...]
    turn = turn_ref[...]
    units = w_gate.shape[0]
    rows_tok = tok_ref[...]
    grad_hidden = dot(grad_ref[...], w_down, ((1,), (1,)))
    high = grad_hidden.astype(BF16)
    rest = grad_hidden - high.astype(F32)
    middle = rest.astype(BF16)
    low = (rest - middle.astype(F32)).astype(BF16)
    pieces = dot(turn, jnp.concatenate([high, middle, low], axis=1), ((1,), (0,)))
    grad_hidden = (
        pieces[:, :units] + pieces[:, units : 2 * units] + pieces[:, 2 * units :]
    )
    pre_gate = dot(rows_tok, w_gate, ((1,), (1,)))
    pre_up = dot(rows_tok, w_up, ((1,), (1,)))
    sigmoid_gate = jax.nn.sigmoid(pre_gate)
    activated = pre_gate * sigmoid_gate
    hidden = (activated * pre_up).astype(BF16)
    grad_gate = (
        grad_hidden * pre_up * sigmoid_gate * (1.0 + pre_gate * (1.0 - sigmoid_gate))
    ).astype(BF16)
    grad_up = (grad_hidden * activated).astype(BF16)
    grad_gate_ref[...] = grad_gate
    grad_up_ref[...] = grad_up
    turned = dot(turn, jnp.concatenate([hidden, grad_gate, grad_up], axis=1), ((0,), (0,)))
    turned = turned.astype(BF16)
    turned_hidden_ref[...] = turned[:, :units]
    din_part = dot(turned[:, units : 2 * units], w_gate, ((1,), (0,)))
    din_part += dot(turned[:, 2 * units :], w_up, ((1,), (0,)))
    din_ref[...] = din_part.astype(BF16)
    out_ref[...] = dot(hidden, w_down, ((1,), (0,))).astype(BF16)


def forward_backward(rows_tok, rows_grad, w_gate, w_up, w_down, turn):
    n_rows, width = rows_tok.shape
    narrow = jax.ShapeDtypeStruct((n_rows, w_gate.shape[0]), BF16)
    wide = jax.ShapeDtypeStruct((n_rows, width), BF16)
    return pl.pallas_call(
        layer_kernel,
        out_shape=(narrow, narrow, narrow, wide, wide),
        compiler_params=pltpu.CompilerParams(vmem_limit_bytes=26 * 1024 * 1024),
        name="layer",
    )(rows_tok, rows_grad, w_gate, w_up, w_down, turn)


def on_device(tokens, cotangent, experts, gate_weights, w_gate, w_up, w_down):
    w_gate, w_up, w_down = w_gate[0], w_up[0], w_down[0]
    width = tokens.shape[1]
    n_z, n_x, n_y = lax.axis_size("z"), lax.axis_size("x"), lax.axis_size("y")
    own_id = lax.axis_index("y")[None].astype(jnp.int32)
    placing, gate_of = slot_tables(experts, gate_weights, own_id)
    placing = placing[0]
    slot_gate = jnp.sum(placing * gate_of[:, 0][None, :], axis=1)
    picks = placing.astype(BF16)
    slot_tokens = dot(picks, tokens, ((1,), (0,))).astype(BF16)
    picked_grad = dot(picks, cotangent, ((1,), (0,)))
    scaled_grad = (picked_grad * slot_gate[:, None]).astype(BF16)

    n_rows = n_x * n_z * C
    quarter = (4 * C, width // 4)
    grad_own = spread(scaled_grad.reshape(quarter), "x").reshape(n_x * C, width)
    grad_own = lax.all_gather(grad_own, "z", axis=0, tiled=True)
    tok_own = spread(slot_tokens.reshape(quarter), "z").reshape(n_z * C, width)
    tok_own = spread(tok_own, "x").reshape(n_rows, width)
    tok_other, grad_other = swap(tok_own), swap(grad_own)

    at_tok = lax.broadcasted_iota(jnp.int32, (n_rows, n_rows), 0)
    at_grad = lax.broadcasted_iota(jnp.int32, (n_rows, n_rows), 1)
    of_z, of_x, of_slot = at_grad // (n_x * C), at_grad // C % n_x, at_grad % C
    turn = (at_tok == of_x * (n_z * C) + of_z * C + of_slot).astype(BF16)

    weights = (w_gate, w_up, w_down, turn)
    hid_a, gg_a, gu_a, out_a, din_a = forward_backward(tok_own, grad_own, *weights)
    tok_other, grad_other, out_a = lax.optimization_barrier((tok_other, grad_other, out_a))
    hid_b, gg_b, gu_b, out_b, din_b = forward_backward(tok_other, grad_other, *weights)

    def chip_sum(mine, partner):
        return (mine.astype(F32) + swap(partner).astype(F32)).astype(BF16)

    sum_din = chip_sum(din_a, din_b)
    sum_out = chip_sum(out_a, out_b).reshape(n_x, n_z * C, width)

    def weight_grad(left_a, right_a, left_b, right_b):
        total = dot(left_a, right_a, ((0,), (0,))) + dot(left_b, right_b, ((0,), (0,)))
        return total.astype(BF16)[None]

    grad_w_gate = weight_grad(gg_a, tok_own, gg_b, tok_other)
    grad_w_up = weight_grad(gu_a, tok_own, gu_b, tok_other)
    grad_w_down = weight_grad(hid_a, grad_own, hid_b, grad_other)

    def exchange_sum(a, axis):
        a = lax.all_to_all(a, axis, split_axis=0, concat_axis=0, tiled=True)
        return jnp.sum(a.astype(F32), axis=0).astype(BF16)

    def turn_sum(a, axis):
        here = lax.axis_index(axis)
        count = a.shape[0]
        total = lax.dynamic_index_in_dim(a, here, keepdims=False).astype(F32)
        for step in (1, count - 1, *range(2, count - 1)):
            theirs = lax.dynamic_index_in_dim(a, (here + step) % count, keepdims=False)
            pairs = [(i, (i + step) % count) for i in range(count)]
            total += lax.ppermute(theirs, axis, pairs).astype(F32)
        return total.astype(BF16)

    sum_din = lax.psum_scatter(sum_din, "z", scatter_dimension=0, tiled=True)
    sum_out = exchange_sum(sum_out, "x")
    sum_out = exchange_sum(sum_out.reshape((n_z,) + quarter), "z").reshape(C, width)
    sum_din = turn_sum(sum_din.reshape((n_x,) + quarter), "x").reshape(C, width)
    sum_z = jnp.concatenate([sum_out, sum_din], axis=0)
    part = width // n_y
    to_y = sum_z.reshape(2 * C, n_y, part).transpose(1, 0, 2)
    by_y = lax.all_to_all(to_y, "y", split_axis=0, concat_axis=0, tiled=True)
    by_y = by_y.reshape(n_y, 2, C, part).astype(F32)

    all_placing, all_gates = slot_tables(
        experts, gate_weights, jnp.arange(n_y, dtype=jnp.int32)
    )
    weighted = all_placing * all_gates.T[:, None, :]
    output = jnp.einsum("ect,ecd->td", weighted, by_y[:, 0], precision=HIGH)
    grad_tokens = jnp.einsum("ect,ecd->td", all_placing, by_y[:, 1], precision=HIGH)
    return (
        output.astype(BF16),
        grad_tokens.astype(BF16),
        grad_w_gate,
        grad_w_up,
        grad_w_down,
    )


def solution(mesh):
    shape = mesh.devices.shape
    fine = Mesh(
        mesh.devices.reshape(shape[0] // 2, 2, shape[1], shape[2]), ("z", "c", "y", "x")
    )
    by_token = ("z", "c", "x")
    return jax.shard_map(
        on_device,
        mesh=fine,
        in_specs=(
            P(by_token, None),
            P(by_token, None),
            P(by_token, None),
            P(by_token, None),
            P("y", by_token, None),
            P("y", by_token, None),
            P("y", by_token, None),
        ),
        out_specs=(
            P(by_token, "y"),
            P(by_token, "y"),
            P("y", by_token, None),
            P("y", by_token, None),
            P("y", by_token, None),
        ),
        check_vma=False,
    )
```

```python
import jax
import jax.numpy as jnp
from jax import lax
from jax.experimental import pallas as pl
from jax.experimental.pallas import tpu as pltpu
from jax.sharding import Mesh, PartitionSpec as P

C = 10
HIGH = lax.Precision.HIGHEST
F32 = jnp.float32
BF16 = jnp.bfloat16


def spread(block, axis):
    count = lax.axis_size(axis)
    copies = jnp.broadcast_to(block[None], (count,) + block.shape)
    return lax.all_to_all(copies, axis, split_axis=0, concat_axis=0, tiled=True)


def swap(a):
    return lax.ppermute(a, "c", [(0, 1), (1, 0)])


def slot_tables(experts, gate_weights, ids):
    chosen = (experts[:, :, None] == ids[None, None, :]).astype(jnp.int32)
    routed = jnp.sum(chosen, axis=1)
    gate_of = jnp.sum(gate_weights[:, :, None] * chosen.astype(F32), axis=1)
    slot_of = jnp.cumsum(routed, axis=0) - routed
    slot_ids = jnp.arange(C, dtype=jnp.int32)
    placing = (
        (slot_of.T[:, None, :] == slot_ids[None, :, None]) & (routed.T[:, None, :] == 1)
    ).astype(F32)
    return placing, gate_of


def dot(a, b, dims):
    return lax.dot_general(a, b, (dims, ((), ())), preferred_element_type=F32)


def layer_kernel(*refs):
    sources, outs, scratch = refs[:6], refs[6:11], refs[11:]
    turned_hidden_ref, grad_gate_ref, grad_up_ref, out_hbm, din_hbm = outs
    tok, grad, w_gate, w_up, w_down, turn_ref, out_ref, din_ref, sems = scratch
    buffers = (tok, grad, w_gate, w_up, w_down, turn_ref)
    loads = [
        pltpu.make_async_copy(source, buffer, sems.at[i])
        for i, (source, buffer) in enumerate(zip(sources, buffers))
    ]
    for i in (1, 4, 5, 0, 2, 3):
        loads[i].start()
    units = w_gate.shape[0]
    loads[1].wait()
    loads[4].wait()
    grad_hidden = dot(grad[...], w_down[...], ((1,), (1,)))
    high = grad_hidden.astype(BF16)
    rest = grad_hidden - high.astype(F32)
    middle = rest.astype(BF16)
    low = (rest - middle.astype(F32)).astype(BF16)
    loads[5].wait()
    turn = turn_ref[...]
    pieces = dot(turn, jnp.concatenate([high, middle, low], axis=1), ((1,), (0,)))
    grad_hidden = (
        pieces[:, :units] + pieces[:, units : 2 * units] + pieces[:, 2 * units :]
    )
    loads[0].wait()
    loads[2].wait()
    pre_gate = dot(tok[...], w_gate[...], ((1,), (1,)))
    loads[3].wait()
    pre_up = dot(tok[...], w_up[...], ((1,), (1,)))
    sigmoid_gate = jax.nn.sigmoid(pre_gate)
    activated = pre_gate * sigmoid_gate
    hidden = (activated * pre_up).astype(BF16)
    grad_gate = (
        grad_hidden * pre_up * sigmoid_gate * (1.0 + pre_gate * (1.0 - sigmoid_gate))
    ).astype(BF16)
    grad_up = (grad_hidden * activated).astype(BF16)
    grad_gate_ref[...] = grad_gate
    grad_up_ref[...] = grad_up
    turned = dot(turn, jnp.concatenate([hidden, grad_gate, grad_up], axis=1), ((0,), (0,)))
    turned = turned.astype(BF16)
    turned_hidden_ref[...] = turned[:, :units]
    din_part = dot(turned[:, units : 2 * units], w_gate[...], ((1,), (0,)))
    din_part += dot(turned[:, 2 * units :], w_up[...], ((1,), (0,)))
    din_ref[...] = din_part.astype(BF16)
    store_din = pltpu.make_async_copy(din_ref, din_hbm, sems.at[6])
    store_din.start()
    out_ref[...] = dot(hidden, w_down[...], ((1,), (0,))).astype(BF16)
    store_out = pltpu.make_async_copy(out_ref, out_hbm, sems.at[7])
    store_out.start()
    store_din.wait()
    store_out.wait()


def forward_backward(rows_tok, rows_grad, w_gate, w_up, w_down, turn):
    n_rows, width = rows_tok.shape
    operands = (rows_tok, rows_grad, w_gate, w_up, w_down, turn)
    operands = [pltpu.with_memory_space_constraint(a, pltpu.HBM) for a in operands]
    narrow = jax.ShapeDtypeStruct((n_rows, w_gate.shape[0]), BF16)
    wide = pltpu.HBM((n_rows, width), BF16)
    in_hbm = pl.BlockSpec(memory_space=pltpu.HBM)
    in_vmem = pl.BlockSpec(memory_space=pltpu.VMEM)
    return pl.pallas_call(
        layer_kernel,
        out_shape=(narrow, narrow, narrow, wide, wide),
        in_specs=[in_hbm] * 6,
        out_specs=(in_vmem, in_vmem, in_vmem, in_hbm, in_hbm),
        scratch_shapes=[
            *(pltpu.VMEM(a.shape, BF16) for a in operands),
            pltpu.VMEM((n_rows, width), BF16),
            pltpu.VMEM((n_rows, width), BF16),
            pltpu.SemaphoreType.DMA((8,)),
        ],
        compiler_params=pltpu.CompilerParams(vmem_limit_bytes=26 * 1024 * 1024),
        name="layer",
    )(*operands)


def on_device(tokens, cotangent, experts, gate_weights, w_gate, w_up, w_down):
    w_gate, w_up, w_down = w_gate[0], w_up[0], w_down[0]
    width = tokens.shape[1]
    n_z, n_x, n_y = lax.axis_size("z"), lax.axis_size("x"), lax.axis_size("y")
    own_id = lax.axis_index("y")[None].astype(jnp.int32)
    placing, gate_of = slot_tables(experts, gate_weights, own_id)
    placing = placing[0]
    slot_gate = jnp.sum(placing * gate_of[:, 0][None, :], axis=1)
    picks = placing.astype(BF16)
    slot_tokens = dot(picks, tokens, ((1,), (0,))).astype(BF16)
    picked_grad = dot(picks, cotangent, ((1,), (0,)))
    scaled_grad = (picked_grad * slot_gate[:, None]).astype(BF16)

    n_rows = n_x * n_z * C
    quarter = (4 * C, width // 4)
    grad_own = spread(scaled_grad.reshape(quarter), "x").reshape(n_x * C, width)
    grad_own = lax.all_gather(grad_own, "z", axis=0, tiled=True)
    tok_own = spread(slot_tokens.reshape(quarter), "z").reshape(n_z * C, width)
    tok_own = spread(tok_own, "x").reshape(n_rows, width)
    tok_other, grad_other = swap(tok_own), swap(grad_own)

    at_tok = lax.broadcasted_iota(jnp.int32, (n_rows, n_rows), 0)
    at_grad = lax.broadcasted_iota(jnp.int32, (n_rows, n_rows), 1)
    of_z, of_x, of_slot = at_grad // (n_x * C), at_grad // C % n_x, at_grad % C
    turn = (at_tok == of_x * (n_z * C) + of_z * C + of_slot).astype(BF16)

    weights = (w_gate, w_up, w_down, turn)
    hid_a, gg_a, gu_a, out_a, din_a = forward_backward(tok_own, grad_own, *weights)
    tok_other, grad_other, out_a = lax.optimization_barrier((tok_other, grad_other, out_a))
    hid_b, gg_b, gu_b, out_b, din_b = forward_backward(tok_other, grad_other, *weights)

    def chip_sum(mine, partner):
        return (mine.astype(F32) + swap(partner).astype(F32)).astype(BF16)

    sum_din = chip_sum(din_a, din_b)
    sum_out = chip_sum(out_a, out_b).reshape(n_x, n_z * C, width)

    def weight_grad(left_a, right_a, left_b, right_b):
        total = dot(left_a, right_a, ((0,), (0,))) + dot(left_b, right_b, ((0,), (0,)))
        return total.astype(BF16)[None]

    grad_w_gate = weight_grad(gg_a, tok_own, gg_b, tok_other)
    grad_w_up = weight_grad(gu_a, tok_own, gu_b, tok_other)
    grad_w_down = weight_grad(hid_a, grad_own, hid_b, grad_other)

    def exchange_sum(a, axis):
        a = lax.all_to_all(a, axis, split_axis=0, concat_axis=0, tiled=True)
        return jnp.sum(a.astype(F32), axis=0).astype(BF16)

    def turn_sum(a, axis):
        here = lax.axis_index(axis)
        count = a.shape[0]
        total = lax.dynamic_index_in_dim(a, here, keepdims=False).astype(F32)
        for step in (1, count - 1, *range(2, count - 1)):
            theirs = lax.dynamic_index_in_dim(a, (here + step) % count, keepdims=False)
            pairs = [(i, (i + step) % count) for i in range(count)]
            total += lax.ppermute(theirs, axis, pairs).astype(F32)
        return total.astype(BF16)

    sum_din = lax.psum_scatter(sum_din, "z", scatter_dimension=0, tiled=True)
    sum_out = exchange_sum(sum_out, "x")
    sum_out, grad_w_gate, grad_w_up, grad_w_down = lax.optimization_barrier(
        (sum_out, grad_w_gate, grad_w_up, grad_w_down)
    )
    sum_out = exchange_sum(sum_out.reshape((n_z,) + quarter), "z").reshape(C, width)
    sum_din = turn_sum(sum_din.reshape((n_x,) + quarter), "x").reshape(C, width)
    sum_z = jnp.concatenate([sum_out, sum_din], axis=0)
    part = width // n_y
    to_y = sum_z.reshape(2 * C, n_y, part).transpose(1, 0, 2)
    by_y = lax.all_to_all(to_y, "y", split_axis=0, concat_axis=0, tiled=True)
    by_y = by_y.reshape(n_y, 2, C, part).astype(F32)

    all_placing, all_gates = slot_tables(
        experts, gate_weights, jnp.arange(n_y, dtype=jnp.int32)
    )
    weighted = all_placing * all_gates.T[:, None, :]
    output = jnp.einsum("ect,ecd->td", weighted, by_y[:, 0], precision=HIGH)
    grad_tokens = jnp.einsum("ect,ecd->td", all_placing, by_y[:, 1], precision=HIGH)
    return (
        output.astype(BF16),
        grad_tokens.astype(BF16),
        grad_w_gate,
        grad_w_up,
        grad_w_down,
    )


def solution(mesh):
    shape = mesh.devices.shape
    fine = Mesh(
        mesh.devices.reshape(shape[0] // 2, 2, shape[1], shape[2]), ("z", "c", "y", "x")
    )
    by_token = ("z", "c", "x")
    return jax.shard_map(
        on_device,
        mesh=fine,
        in_specs=(
            P(by_token, None),
            P(by_token, None),
            P(by_token, None),
            P(by_token, None),
            P("y", by_token, None),
            P("y", by_token, None),
            P("y", by_token, None),
        ),
        out_specs=(
            P(by_token, "y"),
            P(by_token, "y"),
            P("y", by_token, None),
            P("y", by_token, None),
            P("y", by_token, None),
        ),
        check_vma=False,
    )
```

```python
import jax
import jax.numpy as jnp
from jax import lax
from jax.experimental import pallas as pl
from jax.experimental.pallas import tpu as pltpu
from jax.sharding import Mesh, PartitionSpec as P

C = 10
HIGH = lax.Precision.HIGHEST
F32 = jnp.float32
BF16 = jnp.bfloat16


def spread(block, axis):
    count = lax.axis_size(axis)
    copies = jnp.broadcast_to(block[None], (count,) + block.shape)
    return lax.all_to_all(copies, axis, split_axis=0, concat_axis=0, tiled=True)


def swap(a):
    return lax.ppermute(a, "c", [(0, 1), (1, 0)])


def slot_tables(experts, gate_weights, ids):
    chosen = (experts[:, :, None] == ids[None, None, :]).astype(jnp.int32)
    routed = jnp.sum(chosen, axis=1)
    gate_of = jnp.sum(gate_weights[:, :, None] * chosen.astype(F32), axis=1)
    slot_of = jnp.cumsum(routed, axis=0) - routed
    slot_ids = jnp.arange(C, dtype=jnp.int32)
    placing = (
        (slot_of.T[:, None, :] == slot_ids[None, :, None]) & (routed.T[:, None, :] == 1)
    ).astype(F32)
    return placing, gate_of


def dot(a, b, dims):
    return lax.dot_general(a, b, (dims, ((), ())), preferred_element_type=F32)


def layer_kernel(tok_ref, grad_ref, turn_ref, *refs):
    turned_hidden_ref, grad_gate_ref, grad_up_ref, out_ref, din_ref = refs[6:]
    w_gate, w_up, w_down = [
        jnp.concatenate([mine[...], theirs[...]], axis=0)
        for mine, theirs in zip(refs[:3], refs[3:6])
    ]
    turn = turn_ref[...]
    units = w_gate.shape[0]
    rows_tok = tok_ref[...]
    grad_hidden = dot(grad_ref[...], w_down, ((1,), (1,)))
    high = grad_hidden.astype(BF16)
    rest = grad_hidden - high.astype(F32)
    middle = rest.astype(BF16)
    low = (rest - middle.astype(F32)).astype(BF16)
    pieces = dot(turn, jnp.concatenate([high, middle, low], axis=1), ((1,), (0,)))
    grad_hidden = (
        pieces[:, :units] + pieces[:, units : 2 * units] + pieces[:, 2 * units :]
    )
    pre_gate = dot(rows_tok, w_gate, ((1,), (1,)))
    pre_up = dot(rows_tok, w_up, ((1,), (1,)))
    sigmoid_gate = jax.nn.sigmoid(pre_gate)
    activated = pre_gate * sigmoid_gate
    hidden = (activated * pre_up).astype(BF16)
    grad_gate = (
        grad_hidden * pre_up * sigmoid_gate * (1.0 + pre_gate * (1.0 - sigmoid_gate))
    ).astype(BF16)
    grad_up = (grad_hidden * activated).astype(BF16)
    grad_gate_ref[...] = grad_gate
    grad_up_ref[...] = grad_up
    turned = dot(turn, jnp.concatenate([hidden, grad_gate, grad_up], axis=1), ((0,), (0,)))
    turned = turned.astype(BF16)
    turned_hidden_ref[...] = turned[:, :units]
    din_part = dot(turned[:, units : 2 * units], w_gate, ((1,), (0,)))
    din_part += dot(turned[:, 2 * units :], w_up, ((1,), (0,)))
    din_ref[...] = din_part.astype(BF16)
    out_ref[...] = dot(hidden, w_down, ((1,), (0,))).astype(BF16)


def forward_backward(rows_tok, rows_grad, turn, mine, theirs):
    n_rows, width = rows_tok.shape
    narrow = jax.ShapeDtypeStruct((n_rows, 2 * mine[0].shape[0]), BF16)
    wide = jax.ShapeDtypeStruct((n_rows, width), BF16)
    return pl.pallas_call(
        layer_kernel,
        out_shape=(narrow, narrow, narrow, wide, wide),
        compiler_params=pltpu.CompilerParams(vmem_limit_bytes=32 * 1024 * 1024),
        name="layer",
    )(rows_tok, rows_grad, turn, *mine, *theirs)


def on_device(tokens, cotangent, experts, gate_weights, w_gate, w_up, w_down):
    w_gate, w_up, w_down = w_gate[0], w_up[0], w_down[0]
    width = tokens.shape[1]
    n_z, n_x, n_y = lax.axis_size("z"), lax.axis_size("x"), lax.axis_size("y")
    own_id = lax.axis_index("y")[None].astype(jnp.int32)
    placing, gate_of = slot_tables(experts, gate_weights, own_id)
    placing = placing[0]
    slot_gate = jnp.sum(placing * gate_of[:, 0][None, :], axis=1)
    picks = placing.astype(BF16)
    slot_tokens = dot(picks, tokens, ((1,), (0,))).astype(BF16)
    picked_grad = dot(picks, cotangent, ((1,), (0,)))
    scaled_grad = (picked_grad * slot_gate[:, None]).astype(BF16)

    n_rows = n_x * n_z * C
    quarter = (4 * C, width // 4)
    grad_own = spread(scaled_grad.reshape(quarter), "x").reshape(n_x * C, width)
    grad_own = lax.all_gather(grad_own, "z", axis=0, tiled=True)
    tok_own = spread(slot_tokens.reshape(quarter), "z").reshape(n_z * C, width)
    tok_own = spread(tok_own, "x").reshape(n_rows, width)

    at_tok = lax.broadcasted_iota(jnp.int32, (n_rows, n_rows), 0)
    at_grad = lax.broadcasted_iota(jnp.int32, (n_rows, n_rows), 1)
    of_z, of_x, of_slot = at_grad // (n_x * C), at_grad // C % n_x, at_grad % C
    turn = (at_tok == of_x * (n_z * C) + of_z * C + of_slot).astype(BF16)

    mine = (w_gate, w_up, w_down)
    theirs = tuple(swap(w) for w in mine)
    hidden, grad_gate, grad_up, sum_out, sum_din = forward_backward(
        tok_own, grad_own, turn, mine, theirs
    )
    sum_out = sum_out.reshape(n_x, n_z * C, width)

    def weight_grad(left, right):
        units = left.shape[1] // 2
        here = dot(left[:, :units], right, ((0,), (0,)))
        there = swap(dot(left[:, units:], right, ((0,), (0,))))
        return (here + there).astype(BF16)[None]

    grad_w_gate = weight_grad(grad_gate, tok_own)
    grad_w_up = weight_grad(grad_up, tok_own)
    grad_w_down = weight_grad(hidden, grad_own)

    def exchange_sum(a, axis):
        a = lax.all_to_all(a, axis, split_axis=0, concat_axis=0, tiled=True)
        return jnp.sum(a.astype(F32), axis=0).astype(BF16)

    def turn_sum(a, axis):
        here = lax.axis_index(axis)
        count = a.shape[0]
        total = lax.dynamic_index_in_dim(a, here, keepdims=False).astype(F32)
        for step in (1, count - 1, *range(2, count - 1)):
            theirs = lax.dynamic_index_in_dim(a, (here + step) % count, keepdims=False)
            pairs = [(i, (i + step) % count) for i in range(count)]
            total += lax.ppermute(theirs, axis, pairs).astype(F32)
        return total.astype(BF16)

    sum_din = lax.psum_scatter(sum_din, "z", scatter_dimension=0, tiled=True)
    sum_out = exchange_sum(sum_out, "x")
    sum_out = exchange_sum(sum_out.reshape((n_z,) + quarter), "z").reshape(C, width)
    sum_din = turn_sum(sum_din.reshape((n_x,) + quarter), "x").reshape(C, width)
    sum_z = jnp.concatenate([sum_out, sum_din], axis=0)
    part = width // n_y
    to_y = sum_z.reshape(2 * C, n_y, part).transpose(1, 0, 2)
    by_y = lax.all_to_all(to_y, "y", split_axis=0, concat_axis=0, tiled=True)
    by_y = by_y.reshape(n_y, 2, C, part).astype(F32)

    all_placing, all_gates = slot_tables(
        experts, gate_weights, jnp.arange(n_y, dtype=jnp.int32)
    )
    weighted = all_placing * all_gates.T[:, None, :]
    output = jnp.einsum("ect,ecd->td", weighted, by_y[:, 0], precision=HIGH)
    grad_tokens = jnp.einsum("ect,ecd->td", all_placing, by_y[:, 1], precision=HIGH)
    return (
        output.astype(BF16),
        grad_tokens.astype(BF16),
        grad_w_gate,
        grad_w_up,
        grad_w_down,
    )


def solution(mesh):
    shape = mesh.devices.shape
    fine = Mesh(
        mesh.devices.reshape(shape[0] // 2, 2, shape[1], shape[2]), ("z", "c", "y", "x")
    )
    by_token = ("z", "c", "x")
    return jax.shard_map(
        on_device,
        mesh=fine,
        in_specs=(
            P(by_token, None),
            P(by_token, None),
            P(by_token, None),
            P(by_token, None),
            P("y", by_token, None),
            P("y", by_token, None),
            P("y", by_token, None),
        ),
        out_specs=(
            P(by_token, "y"),
            P(by_token, "y"),
            P("y", by_token, None),
            P("y", by_token, None),
            P("y", by_token, None),
        ),
        check_vma=False,
    )
```

```python
import jax
import jax.numpy as jnp
from jax import lax
from jax.experimental import pallas as pl
from jax.experimental.pallas import tpu as pltpu
from jax.sharding import Mesh, PartitionSpec as P

C = 10
HIGH = lax.Precision.HIGHEST
F32 = jnp.float32
BF16 = jnp.bfloat16


def spread(block, axis):
    count = lax.axis_size(axis)
    copies = jnp.broadcast_to(block[None], (count,) + block.shape)
    return lax.all_to_all(copies, axis, split_axis=0, concat_axis=0, tiled=True)


def swap(a):
    return lax.ppermute(a, "c", [(0, 1), (1, 0)])


def slot_tables(experts, gate_weights, ids):
    chosen = (experts[:, :, None] == ids[None, None, :]).astype(jnp.int32)
    routed = jnp.sum(chosen, axis=1)
    gate_of = jnp.sum(gate_weights[:, :, None] * chosen.astype(F32), axis=1)
    slot_of = jnp.cumsum(routed, axis=0) - routed
    slot_ids = jnp.arange(C, dtype=jnp.int32)
    placing = (
        (slot_of.T[:, None, :] == slot_ids[None, :, None]) & (routed.T[:, None, :] == 1)
    ).astype(F32)
    return placing, gate_of


def dot(a, b, dims):
    return lax.dot_general(a, b, (dims, ((), ())), preferred_element_type=F32)


def layer_kernel(tok_ref, grad_ref, turn_ref, *refs):
    sources, outs, scratch = refs[:6], refs[6:11], refs[11:]
    turned_hidden_ref, grad_gate_ref, grad_up_ref, out_hbm, din_hbm = outs
    w_gate, w_up, w_down, out_ref, din_ref, sems = scratch
    half = w_gate.shape[0] // 2
    loads = [
        pltpu.make_async_copy(
            source, (w_gate, w_up, w_down)[i % 3].at[pl.ds(i // 3 * half, half)], sems.at[i]
        )
        for i, source in enumerate(sources)
    ]
    for i in (2, 5, 0, 3, 1, 4):
        loads[i].start()
    turn = turn_ref[...]
    units = 2 * half
    loads[2].wait()
    loads[5].wait()
    grad_hidden = dot(grad_ref[...], w_down[...], ((1,), (1,)))
    high = grad_hidden.astype(BF16)
    rest = grad_hidden - high.astype(F32)
    middle = rest.astype(BF16)
    low = (rest - middle.astype(F32)).astype(BF16)
    pieces = dot(turn, jnp.concatenate([high, middle, low], axis=1), ((1,), (0,)))
    grad_hidden = (
        pieces[:, :units] + pieces[:, units : 2 * units] + pieces[:, 2 * units :]
    )
    loads[0].wait()
    loads[3].wait()
    pre_gate = dot(tok_ref[...], w_gate[...], ((1,), (1,)))
    loads[1].wait()
    loads[4].wait()
    pre_up = dot(tok_ref[...], w_up[...], ((1,), (1,)))
    sigmoid_gate = jax.nn.sigmoid(pre_gate)
    activated = pre_gate * sigmoid_gate
    hidden = (activated * pre_up).astype(BF16)
    grad_gate = (
        grad_hidden * pre_up * sigmoid_gate * (1.0 + pre_gate * (1.0 - sigmoid_gate))
    ).astype(BF16)
    grad_up = (grad_hidden * activated).astype(BF16)
    grad_gate_ref[...] = grad_gate
    grad_up_ref[...] = grad_up
    turned = dot(turn, jnp.concatenate([hidden, grad_gate, grad_up], axis=1), ((0,), (0,)))
    turned = turned.astype(BF16)
    turned_hidden_ref[...] = turned[:, :units]
    din_part = dot(turned[:, units : 2 * units], w_gate[...], ((1,), (0,)))
    din_part += dot(turned[:, 2 * units :], w_up[...], ((1,), (0,)))
    din_ref[...] = din_part.astype(BF16)
    store_din = pltpu.make_async_copy(din_ref, din_hbm, sems.at[6])
    store_din.start()
    out_ref[...] = dot(hidden, w_down[...], ((1,), (0,))).astype(BF16)
    store_out = pltpu.make_async_copy(out_ref, out_hbm, sems.at[7])
    store_out.start()
    store_din.wait()
    store_out.wait()


def forward_backward(rows_tok, rows_grad, turn, mine, theirs):
    n_rows, width = rows_tok.shape
    units = 2 * mine[0].shape[0]
    weights = [pltpu.with_memory_space_constraint(w, pltpu.HBM) for w in (*mine, *theirs)]
    narrow = jax.ShapeDtypeStruct((n_rows, units), BF16)
    wide = pltpu.HBM((n_rows, width), BF16)
    in_hbm = pl.BlockSpec(memory_space=pltpu.HBM)
    in_vmem = pl.BlockSpec(memory_space=pltpu.VMEM)
    return pl.pallas_call(
        layer_kernel,
        out_shape=(narrow, narrow, narrow, wide, wide),
        in_specs=[in_vmem] * 3 + [in_hbm] * 6,
        out_specs=(in_vmem, in_vmem, in_vmem, in_hbm, in_hbm),
        scratch_shapes=[
            *(pltpu.VMEM((units, width), BF16) for _ in range(3)),
            pltpu.VMEM((n_rows, width), BF16),
            pltpu.VMEM((n_rows, width), BF16),
            pltpu.SemaphoreType.DMA((8,)),
        ],
        compiler_params=pltpu.CompilerParams(vmem_limit_bytes=32 * 1024 * 1024),
        name="layer",
    )(rows_tok, rows_grad, turn, *weights)


def on_device(tokens, cotangent, experts, gate_weights, w_gate, w_up, w_down):
    w_gate, w_up, w_down = w_gate[0], w_up[0], w_down[0]
    width = tokens.shape[1]
    n_z, n_x, n_y = lax.axis_size("z"), lax.axis_size("x"), lax.axis_size("y")
    own_id = lax.axis_index("y")[None].astype(jnp.int32)
    placing, gate_of = slot_tables(experts, gate_weights, own_id)
    placing = placing[0]
    slot_gate = jnp.sum(placing * gate_of[:, 0][None, :], axis=1)
    picks = placing.astype(BF16)
    slot_tokens = dot(picks, tokens, ((1,), (0,))).astype(BF16)
    picked_grad = dot(picks, cotangent, ((1,), (0,)))
    scaled_grad = (picked_grad * slot_gate[:, None]).astype(BF16)

    n_rows = n_x * n_z * C
    quarter = (4 * C, width // 4)
    grad_own = spread(scaled_grad.reshape(quarter), "x").reshape(n_x * C, width)
    grad_own = lax.all_gather(grad_own, "z", axis=0, tiled=True)
    tok_own = spread(slot_tokens.reshape(quarter), "z").reshape(n_z * C, width)
    tok_own = spread(tok_own, "x").reshape(n_rows, width)

    at_tok = lax.broadcasted_iota(jnp.int32, (n_rows, n_rows), 0)
    at_grad = lax.broadcasted_iota(jnp.int32, (n_rows, n_rows), 1)
    of_z, of_x, of_slot = at_grad // (n_x * C), at_grad // C % n_x, at_grad % C
    turn = (at_tok == of_x * (n_z * C) + of_z * C + of_slot).astype(BF16)

    mine = (w_gate, w_up, w_down)
    theirs = tuple(swap(w) for w in mine)
    hidden, grad_gate, grad_up, sum_out, sum_din = forward_backward(
        tok_own, grad_own, turn, mine, theirs
    )
    sum_out = sum_out.reshape(n_x, n_z * C, width)

    def weight_grad(left, right):
        units = left.shape[1] // 2
        here = dot(left[:, :units], right, ((0,), (0,)))
        there = swap(dot(left[:, units:], right, ((0,), (0,))))
        return (here + there).astype(BF16)[None]

    grad_w_gate = weight_grad(grad_gate, tok_own)
    grad_w_up = weight_grad(grad_up, tok_own)
    grad_w_down = weight_grad(hidden, grad_own)

    def exchange_sum(a, axis):
        a = lax.all_to_all(a, axis, split_axis=0, concat_axis=0, tiled=True)
        return jnp.sum(a.astype(F32), axis=0).astype(BF16)

    def turn_sum(a, axis):
        here = lax.axis_index(axis)
        count = a.shape[0]
        total = lax.dynamic_index_in_dim(a, here, keepdims=False).astype(F32)
        for step in (1, count - 1, *range(2, count - 1)):
            theirs = lax.dynamic_index_in_dim(a, (here + step) % count, keepdims=False)
            pairs = [(i, (i + step) % count) for i in range(count)]
            total += lax.ppermute(theirs, axis, pairs).astype(F32)
        return total.astype(BF16)

    sum_din = lax.psum_scatter(sum_din, "z", scatter_dimension=0, tiled=True)
    sum_out = exchange_sum(sum_out, "x")
    sum_out = exchange_sum(sum_out.reshape((n_z,) + quarter), "z").reshape(C, width)
    sum_din = turn_sum(sum_din.reshape((n_x,) + quarter), "x").reshape(C, width)
    sum_z = jnp.concatenate([sum_out, sum_din], axis=0)
    part = width // n_y
    to_y = sum_z.reshape(2 * C, n_y, part).transpose(1, 0, 2)
    by_y = lax.all_to_all(to_y, "y", split_axis=0, concat_axis=0, tiled=True)
    by_y = by_y.reshape(n_y, 2, C, part).astype(F32)

    all_placing, all_gates = slot_tables(
        experts, gate_weights, jnp.arange(n_y, dtype=jnp.int32)
    )
    weighted = all_placing * all_gates.T[:, None, :]
    output = jnp.einsum("ect,ecd->td", weighted, by_y[:, 0], precision=HIGH)
    grad_tokens = jnp.einsum("ect,ecd->td", all_placing, by_y[:, 1], precision=HIGH)
    return (
        output.astype(BF16),
        grad_tokens.astype(BF16),
        grad_w_gate,
        grad_w_up,
        grad_w_down,
    )


def solution(mesh):
    shape = mesh.devices.shape
    fine = Mesh(
        mesh.devices.reshape(shape[0] // 2, 2, shape[1], shape[2]), ("z", "c", "y", "x")
    )
    by_token = ("z", "c", "x")
    return jax.shard_map(
        on_device,
        mesh=fine,
        in_specs=(
            P(by_token, None),
            P(by_token, None),
            P(by_token, None),
            P(by_token, None),
            P("y", by_token, None),
            P("y", by_token, None),
            P("y", by_token, None),
        ),
        out_specs=(
            P(by_token, "y"),
            P(by_token, "y"),
            P("y", by_token, None),
            P("y", by_token, None),
            P("y", by_token, None),
        ),
        check_vma=False,
    )
```
